256 devices in a mesh: grp: 16 (over z_lo, y, core), seq: 16 (over z_hi, x).
Axes of the slice: x: 4, y: 4, z: 8 (z_hi: 4, z_lo: 2; z = z_hi * 2 + z_lo), core: 2. Of those that a mesh axis runs over, the one named last changes fastest.
Arguments:
- query: bfloat16 [16, 4096, 640], P('grp', 'seq'), may hold values from -64 to 64
- resp_kv: bfloat16 [16, 4096, 256], P('grp', 'seq'), may hold values from -6 to 6
- prompt_kv: bfloat16 [16, 4096, 256], P('grp', 'seq'), may hold values from -64 to 64
- grad_out: bfloat16 [16, 4096, 640], P('grp', 'seq'), may hold values from -6 to 6
- rewards: float32 [16, 16], P('grp'), may hold values from -4 to 4
- lengths: int32 [16, 16], P('grp'), may hold values from 1 to 256, as said below
- block_order: int32 [16, 32], P('grp'), may hold values from 0 to 31, each once within a row
Outputs:
- grad_query: bfloat16 [16, 4096, 640], P('grp', 'seq')
- grad_stream: bfloat16 [16, 4096, 256], P('grp', 'seq')
- grad_prompt: bfloat16 [16, 4096, 256], P('grp', 'seq')
The draws below stay inside these ranges and needn't reach their ends.
Inputs may be any that keep to these rules, and one draw needn't show every extreme that they name: `lengths`: each response has 1 to 256 tokens; some response has exactly 256. Each row of block_order names every response block of its group once.
All inputs are finite; a program needn't handle non-finite values.
Results may differ from the reference program's by a relative error of at most 0.015.
Values may be sent and summed in bfloat16 or wider, within the bound.
A program may use at most 128 MiB of HBM per device.

```python
import jax
import jax.numpy as jnp
from jax import lax

HD = 128
QPK = 5
RESP = 16
BLK = 128
NB = 2
GROUPS = 16
PROMPT = 4096
NBLK = 32
STREAM = 4096


def draw_query(key, part):
    base_draw = jnp.clip(jax.random.normal(jax.random.fold_in(key, 1), (GROUPS, STREAM, QPK * HD), jnp.float32), -6.0, 6.0)
    return jnp.clip(base_draw, -64.0, 64.0).astype(jnp.bfloat16)


def draw_prompt_kv(key, part):
    base_draw = jnp.clip(jax.random.normal(jax.random.fold_in(key, 2), (GROUPS, PROMPT, 2 * HD), jnp.float32), -6.0, 6.0)
    return jnp.clip(base_draw, -64.0, 64.0).astype(jnp.bfloat16)


def draw_lengths(key, part):
    group_index = jnp.arange(GROUPS, dtype=jnp.int32)
    upper_len = jnp.maximum(NB * BLK * (GROUPS + 2 * group_index) // (3 * GROUPS - 2), 1)
    raw_bits = jax.random.randint(jax.random.fold_in(key, 5), (GROUPS, RESP), 0, 1 << 20, jnp.int32)
    half_span = (upper_len + 1) // 2
    drawn_lengths = upper_len[:, None] - raw_bits % half_span[:, None]
    full_slot = jax.random.randint(jax.random.fold_in(key, 6), (), 0, RESP, jnp.int32)
    drawn_lengths = drawn_lengths.at[GROUPS - 1, full_slot].set(NB * BLK)
    return drawn_lengths.astype(jnp.int32)


def block_scale(key, dims, cuts, least, top_value):
    def one(dim, blocks):
        heights = jax.random.uniform(jax.random.fold_in(jax.random.fold_in(key, 6), dim), (blocks,), jnp.float32, least / len(cuts), top_value / len(cuts))
        return jnp.repeat(jnp.exp(heights), dims[dim] // blocks).reshape((-1,) + (1,) * (len(dims) - dim - 1))

    level = one(*cuts[0])
    for cut in cuts[1:]:
        level = level * one(*cut)
    return level


def noise(rng, extent, scale, bound, cuts=(), kind=jnp.bfloat16):
    factor_of = block_scale(rng, extent, cuts, -0.22, 0.18) if cuts else 1.0
    values = jax.random.normal(rng, extent, jnp.float32) * scale * factor_of
    return jnp.minimum(jnp.maximum(values, -bound), bound).astype(kind)


def setup_inputs(seed: int = 0) -> dict:
    keys = jax.random.split(jax.random.key(seed), 8)
    return {
        "query": draw_query(jax.random.fold_in(keys[7], 71), 0),
        "resp_kv": noise(keys[1], (GROUPS, STREAM, 2 * HD), 1.0, 6.0, ((0, 16), (1, 16))),
        "prompt_kv": draw_prompt_kv(jax.random.fold_in(keys[7], 71), 0),
        "grad_out": noise(keys[3], (GROUPS, STREAM, QPK * HD), 1.0, 6.0, ((0, 16), (1, 16))),
        "rewards": noise(keys[4], (GROUPS, RESP), 1.0, 4.0, ((0, 16),), jnp.float32),
        "lengths": draw_lengths(jax.random.fold_in(keys[7], 71), 0),
        "block_order": jax.vmap(lambda own: jax.random.permutation(own, NBLK))(jax.random.split(keys[6], GROUPS)).reshape((GROUPS, NBLK)).astype(jnp.int32),
    }


LOSS_SCALE = 32.0
BIG_NEGATIVE = -1e30


def rounded(values):
    return lax.optimization_barrier(values.astype(jnp.bfloat16)).astype(jnp.float32)


def block_grads(query_block, weighted, prompt_pairs, own_pairs, positions):
    half_width = prompt_pairs.shape[1] // 2
    score_scale = half_width ** -0.5
    query_wide = query_block.astype(jnp.float32)
    prompt_keys = prompt_pairs[:, :half_width].astype(jnp.float32)
    prompt_values = prompt_pairs[:, half_width:].astype(jnp.float32)
    own_keys = own_pairs[:, :half_width].astype(jnp.float32)
    own_values = own_pairs[:, half_width:].astype(jnp.float32)
    visible = (jnp.arange(own_pairs.shape[0], dtype=jnp.int32)[None, :] <= positions[:, None])[None]
    scores_prompt = jnp.einsum("thd,kd->htk", query_wide, prompt_keys) * score_scale
    scores_own = jnp.where(visible, jnp.einsum("thd,kd->htk", query_wide, own_keys) * score_scale, BIG_NEGATIVE)
    peak_score = jnp.maximum(jnp.max(scores_prompt, axis=2), jnp.max(scores_own, axis=2))
    expo_prompt = jnp.exp(scores_prompt - peak_score[..., None])
    expo_own = jnp.where(visible, jnp.exp(scores_own - peak_score[..., None]), 0.0)
    prob_total = jnp.sum(expo_prompt, axis=2) + jnp.sum(expo_own, axis=2)
    probs_prompt = expo_prompt / prob_total[..., None]
    probs_own = expo_own / prob_total[..., None]
    low_prompt = rounded(probs_prompt)
    low_own = rounded(probs_own)
    attended = jnp.einsum("htk,kd->thd", low_prompt, prompt_values) + jnp.einsum("htk,kd->thd", low_own, own_values)
    row_delta = jnp.einsum("thd,thd->ht", weighted, attended)
    grad_prompt_scores = rounded(probs_prompt * (jnp.einsum("thd,kd->htk", weighted, prompt_values) - row_delta[..., None]))
    grad_own_scores = rounded(probs_own * (jnp.einsum("thd,kd->htk", weighted, own_values) - row_delta[..., None]))
    grad_query = (jnp.einsum("htk,kd->thd", grad_prompt_scores, prompt_keys) + jnp.einsum("htk,kd->thd", grad_own_scores, own_keys)) * score_scale
    prompt_term = jnp.concatenate([jnp.einsum("htk,thd->kd", grad_prompt_scores, query_wide) * score_scale, jnp.einsum("htk,thd->kd", low_prompt, weighted)], axis=1)
    own_term = jnp.concatenate([jnp.einsum("htk,thd->kd", grad_own_scores, query_wide) * score_scale, jnp.einsum("htk,thd->kd", low_own, weighted)], axis=1)
    return grad_query, prompt_term, own_term


def reference(query, resp_kv, prompt_kv, grad_out, rewards, lengths, block_order):
    count = jnp.sum(lengths).astype(jnp.float32)
    advantage = rewards - jnp.mean(rewards, axis=1, keepdims=True)
    factor = advantage * (LOSS_SCALE * GROUPS * RESP * NB * BLK) / count

    def one_group(group_inputs):
        group_query, group_pairs, group_prompt, group_grad, group_factor, group_lengths, block_plan = group_inputs
        inverse = jnp.argsort(block_plan).astype(jnp.int32)
        blocks = group_pairs.reshape(RESP * NB, BLK, 2 * HD)

        def block_step(carried, block_index):
            prompt_sum, stream_sum = carried
            stream_block = block_plan[block_index]
            response = stream_block // NB
            first_row = (stream_block % NB) * BLK
            slot_index = lax.dynamic_slice_in_dim(inverse, response * NB, NB)
            own_pairs = jnp.take(blocks, slot_index, axis=0).reshape(NB * BLK, 2 * HD)
            start_row = (block_index * BLK).astype(jnp.int32)
            query_block = lax.dynamic_slice_in_dim(group_query, start_row, BLK).reshape(BLK, QPK, HD)
            grad_block = lax.dynamic_slice_in_dim(group_grad, start_row, BLK)
            positions = first_row + jnp.arange(BLK, dtype=jnp.int32)
            token_weight = jnp.where(positions < group_lengths[response], group_factor[response], 0.0)
            weighted = rounded(grad_block.astype(jnp.float32) * token_weight[:, None]).reshape(BLK, QPK, HD)
            grad_query, prompt_term, own_term = block_grads(query_block, weighted, group_prompt, own_pairs, positions)
            stream_sum = stream_sum.at[slot_index].add(own_term.reshape(NB, BLK, 2 * HD))
            return (prompt_sum + prompt_term, stream_sum), grad_query.reshape(BLK, QPK * HD).astype(jnp.bfloat16)

        initial = (jnp.zeros((PROMPT, 2 * HD), jnp.float32), jnp.zeros((RESP * NB, BLK, 2 * HD), jnp.float32))
        (prompt_sum, stream_sum), grad_rows = lax.scan(block_step, initial, jnp.arange(RESP * NB, dtype=jnp.int32))
        return (grad_rows.reshape(STREAM, QPK * HD), stream_sum.reshape(STREAM, 2 * HD).astype(jnp.bfloat16), prompt_sum.astype(jnp.bfloat16))

    grad_query, grad_stream, grad_prompt = lax.map(one_group, (query, resp_kv, prompt_kv, grad_out, factor, lengths, block_order))
    return (grad_query, grad_stream, grad_prompt)
```

```python
import jax
import jax.numpy as jnp
from jax import lax
from jax.experimental import pallas as pl
from jax.experimental.pallas import tpu as pltpu
from jax.sharding import PartitionSpec as P

RESP = 16
BLK = 128
NB = 2
HD = 128
QPK = 5
LOSS_SCALE = 32.0
NEG = -1e30
LOG2E = 1.4426950408889634
MESH = pl.DeviceIdType.MESH
F32 = jnp.float32
BF16 = jnp.bfloat16

SIDE = 4
MEMBERS = SIDE * SIDE
CHUNK = NB * BLK
ROWS = NB * QPK * BLK
TILES = NB * QPK
WIDE = 256

UP = pl.ds(0, BLK)
DOWN = pl.ds(BLK, BLK)
KEYS = pl.ds(0, HD)
VALUES = pl.ds(HD, HD)
OWN = MEMBERS

GATHER_ORDER = (
    (0, 0), (0, 1), (0, 3), (0, 2), (3, 0), (1, 0), (1, 1), (1, 3),
    (3, 1), (3, 3), (2, 0), (2, 1), (2, 3), (3, 2), (1, 2), (2, 2),
)
REDUCE_ORDER = (
    (2, 2), (3, 2), (1, 2), (2, 1), (2, 3), (2, 0), (1, 1), (3, 1),
    (1, 3), (3, 3), (1, 0), (3, 0), (0, 2), (0, 1), (0, 3), (0, 0),
)
N_COPIES = 58


def dot(a, b):
    return jnp.dot(a, b, preferred_element_type=F32)


def wrapped(t, n):
    return t - jnp.where(t >= n, n, 0)


def slot_at(sequence, step):
    slot = jnp.int32(0)
    for k, (a, b) in enumerate(sequence):
        slot = slot + jnp.where(step == k, a * SIDE + b, 0)
    return slot


def kernel(
    query_hbm, resp_hbm, prompt_hbm, grad_out_hbm, rewards_hbm, lengths_hbm, order_hbm,
    grad_query, grad_stream, grad_prompt,
    query, grad_out, resp, rewards, lengths, order, partner,
    kv, scores, dprobs, q_rows, w_rows, q_cols, w_cols,
    peak, total, weigh, p_low, ds_low, dq_cols, g_tmp, g_send, g_hold,
    x_rel_a, x_rel_b, x_in_l, x_in_r, x_sum,
    z_send, z_rel_a, z_rel_b, z_in_l, z_in_r, z_far,
    table_a, send_b, partner_kv, table_c, send_d, partner_grad, give, own_grad,
    count_send, count_recv,
    ssem, rsem, esend, erecv, csend, crecv, isem, known,
):
    scale = HD ** (-0.5)
    c = scale * LOG2E
    me = lax.axis_index("seq")
    grp = lax.axis_index("grp")
    z, x = me // SIDE, me % SIDE
    right = z * SIDE + (x + 1) % SIDE
    left = z * SIDE + (x + SIDE - 1) % SIDE
    above = ((z + 1) % SIDE) * SIDE + x
    below = ((z + SIDE - 1) % SIDE) * SIDE + x

    inputs = [
        pltpu.make_async_copy(src, dst, isem.at[k])
        for k, (src, dst) in enumerate((
            (prompt_hbm, kv.at[0]), (resp_hbm, resp), (order_hbm, order), (lengths_hbm, lengths),
            (rewards_hbm, rewards), (query_hbm, query), (grad_out_hbm, grad_out),
        ))
    ]
    for load in inputs:
        load.start()

    copies = {}

    def declare(name, src, dst, dev):
        k = len(copies)
        copies[name] = pltpu.make_async_remote_copy(
            src_ref=src, dst_ref=dst, send_sem=ssem.at[k], recv_sem=rsem.at[k],
            device_id={"seq": dev}, device_id_type=MESH,
        )

    def slot_ref(a, b, half):
        return kv.at[a * SIDE + b, half]

    halves = (UP, DOWN)
    for a in range(SIDE):
        for h in range(2):
            declare(("R", a, h), slot_ref(a, 0, halves[h]), slot_ref(a, 3, halves[h]), right)
            declare(("L", a, h), slot_ref(a, 0, halves[h]), slot_ref(a, 1, halves[h]), left)
            declare(("gr", a, h), g_send.at[a * SIDE + 1, halves[h]], x_in_l.at[a, halves[h]], right)
            declare(("gl", a, h), g_send.at[a * SIDE + 3, halves[h]], x_in_r.at[a, halves[h]], left)
        if a != 1:
            declare(("FR", a), slot_ref(a, 3, UP), slot_ref(a, 2, UP), right)
        if a != 3:
            declare(("FL", a), slot_ref(a, 1, DOWN), slot_ref(a, 2, DOWN), left)
        if a % 2 == 0:
            declare(("r", a), g_send.at[a * SIDE + 2, UP], x_rel_a.at[a // 2], right)
            declare(("l", a), g_send.at[a * SIDE + 2, DOWN], x_rel_b.at[a // 2], left)
    for h in range(2):
        declare(("U", h), slot_ref(0, 0, halves[h]), slot_ref(3, 0, halves[h]), above)
        declare(("D", h), slot_ref(0, 0, halves[h]), slot_ref(1, 0, halves[h]), below)
        declare(("zu", h), z_send.at[1, halves[h]], z_in_l.at[halves[h]], above)
        declare(("zd", h), z_send.at[3, halves[h]], z_in_r.at[halves[h]], below)
    declare(("VU",), slot_ref(0, 2, DOWN), slot_ref(3, 2, DOWN), above)
    declare(("VD",), slot_ref(0, 2, UP), slot_ref(1, 2, UP), below)
    declare(("yu",), g_send.at[SIDE + 2], z_far.at[0], above)
    declare(("yd",), g_send.at[3 * SIDE + 2], z_far.at[1], below)
    declare(("FU",), slot_ref(3, 0, UP), slot_ref(2, 0, UP), above)
    declare(("FD",), slot_ref(1, 0, DOWN), slot_ref(2, 0, DOWN), below)
    declare(("zr",), z_send.at[2, UP], z_rel_a, above)
    declare(("zl",), z_send.at[2, DOWN], z_rel_b, below)

    def start(*names):
        for name in names:
            copies[name].start()

    def arrived(*names):
        for name in names:
            copies[name].wait_recv()

    def piece(t):
        second = jnp.where(t >= MEMBERS // 2, 1, 0)
        return (
            slice(None),
            pl.ds(pl.multiple_of((t - second * (MEMBERS // 2)) * 16, 16), 16),
            pl.ds(pl.multiple_of(second * HD, HD), HD),
        )

    def spread_copy(stage, src, dst, k):
        t = wrapped(me + k, MEMBERS)
        return pltpu.make_async_remote_copy(
            src_ref=src.at[piece(t)], dst_ref=dst.at[pl.ds(NB * k, NB)],
            send_sem=esend.at[stage, k], recv_sem=erecv.at[stage, k],
            device_id={"seq": t}, device_id_type=MESH,
        )

    def deliver_copy(stage, src, dst, k):
        t = wrapped(me + k, MEMBERS)
        return pltpu.make_async_remote_copy(
            src_ref=src.at[pl.ds(NB * k, NB)], dst_ref=dst.at[piece(me)],
            send_sem=esend.at[stage, k], recv_sem=erecv.at[stage, k],
            device_id={"seq": t}, device_id_type=MESH,
        )

    def every(fn):
        def body(k, carry):
            fn(k)
            return carry

        lax.fori_loop(1, MEMBERS, body, 0)

    def spread(stage, src, dst):
        every(lambda k: spread_copy(stage, src, dst, k).start())
        dst[pl.ds(0, NB)] = src[piece(me)]

    def deliver(stage, table, buf, dst):
        def fill(k, carry):
            for i in range(NB):
                buf[NB * k + i] = table[partner[NB * wrapped(me + k, MEMBERS) + i]]
            return carry

        lax.fori_loop(0, MEMBERS, fill, 0)
        every(lambda k: deliver_copy(stage, buf, dst, k).start())
        dst[piece(me)] = buf[pl.ds(0, NB)]

    def find_partners():
        def one(j, carry):
            b = order[j]
            sibling = b + 1 - 2 * lax.rem(b, NB)
            found = jnp.int32(0)
            for k in range(MEMBERS):
                far = wrapped(me + MEMBERS - k, MEMBERS) * NB
                for i in range(NB):
                    found = found + jnp.where(order[NB * k + i] == sibling, far + i, 0)
            partner[j] = found
            return carry

        lax.fori_loop(0, NB * MEMBERS, one, 0)

    mate = grp + 1 - 2 * (grp % 2)
    y_next = (grp // 8) * 8 + (grp % 8 + 2) % 8
    y_last = (grp // 8) * 8 + (grp % 8 + 6) % 8
    z_mate = (grp + 8) % 16
    counts = [
        pltpu.make_async_remote_copy(
            src_ref=src, dst_ref=count_recv.at[k], send_sem=csend.at[k], recv_sem=crecv.at[k],
            device_id={"grp": peer}, device_id_type=MESH,
        )
        for k, (src, peer) in enumerate((
            (count_send.at[0], mate), (count_send.at[1], y_next), (count_send.at[1], y_last),
            (count_recv.at[1], y_next), (count_send.at[2], z_mate),
        ))
    ]

    neighbours = (right, left, above, below)
    barrier = pltpu.get_barrier_semaphore()
    for dev in neighbours:
        pl.semaphore_signal(barrier, inc=1, device_id={"seq": dev}, device_id_type=MESH)
    for dev in (mate, y_next, y_last, z_mate):
        pl.semaphore_signal(barrier, inc=1, device_id={"grp": dev}, device_id_type=MESH)

    def pass_on(k):
        for dev in neighbours:
            pl.semaphore_signal(known.at[k], inc=1, device_id={"seq": dev}, device_id_type=MESH)

    def heard(k):
        pl.semaphore_wait(known.at[k], len(neighbours))

    inputs[0].wait()
    pl.semaphore_wait(barrier, 8)

    start(("U", 0), ("D", 1), ("R", 0, 0), ("L", 0, 1), ("U", 1), ("D", 0), ("R", 0, 1), ("L", 0, 0))
    pass_on(0)
    for load in inputs[1:]:
        load.wait()
    tokens = lengths[0]
    for r in range(1, RESP):
        tokens = tokens + lengths[r]
    count_send[0] = jnp.full((8, HD), tokens, jnp.int32)
    counts[0].start()
    heard(0)
    pass_on(1)

    mean = rewards[0]
    for r in range(1, RESP):
        mean = mean + rewards[r]
    mean = mean * (1.0 / RESP)
    is_later = []
    row_number = lax.broadcasted_iota(jnp.int32, (BLK, HD), 0)
    for i in range(NB):
        b = order[NB * me + i]
        r, h = b // NB, b % NB
        is_later.append(h)
        gain = jnp.where(row_number + h * BLK < lengths[r], rewards[r] - mean, 0.0)
        for head in range(QPK):
            tile = pl.ds((i * QPK + head) * BLK, BLK)
            rows = pl.ds(i * BLK, BLK)
            cols = pl.ds(head * HD, HD)
            q = query[rows, cols].astype(F32)
            w = grad_out[rows, cols].astype(F32) * gain
            q_rows[tile, :] = q.astype(BF16)
            w_rows[tile, :] = w.astype(BF16)
            q_cols[:, tile] = q.T.astype(BF16)
            w_cols[:, tile] = w.T.astype(BF16)
    heard(1)
    pass_on(2)
    find_partners()
    peak[...] = jnp.full_like(peak, NEG)
    total[...] = jnp.zeros_like(total)
    weigh[...] = jnp.zeros_like(weigh)
    dq_cols[...] = jnp.zeros_like(dq_cols)

    def take_in(slot):
        for n in range(TILES):
            tile = pl.ds(n * BLK, BLK)
            s = scores[slot, :, tile].reshape(CHUNK // 8, 8, BLK)
            d = dprobs[slot, :, tile].reshape(CHUNK // 8, 8, BLK)
            before = peak[:, tile]
            now = jnp.maximum(before, jnp.max(s, axis=0))
            fade = jnp.exp2((before - now) * c)
            e = jnp.exp2((s - now[None]) * c)
            total[:, tile] = total[:, tile] * fade + jnp.sum(e, axis=0)
            weigh[:, tile] = weigh[:, tile] * fade + jnp.sum(e * d, axis=0)
            peak[:, tile] = now

    def own_pair(i, cols):
        return jnp.concatenate([resp[i, :, cols], partner_kv[i, :, cols]], axis=0)

    def own_scores():
        key = lax.broadcasted_iota(jnp.int32, (CHUNK, BLK), 0)
        pos = lax.broadcasted_iota(jnp.int32, (CHUNK, BLK), 1)
        for i in range(NB):
            limit = jnp.where(is_later[i] == 1, CHUNK, BLK)
            seen = jnp.where(key < BLK, pos - key, limit - 1 - key) >= 0
            k_own, v_own = own_pair(i, KEYS), own_pair(i, VALUES)
            for head in range(QPK):
                tile = pl.ds((i * QPK + head) * BLK, BLK)
                scores[OWN, :, tile] = jnp.where(seen, dot(k_own, q_cols[:, tile]), NEG)
                dprobs[OWN, :, tile] = dot(v_own, w_cols[:, tile])
        take_in(OWN)

    def gather_events(s):
        if s == 1:
            arrived(("R", 0, 0), ("L", 0, 1))
            start(("FR", 0), ("FL", 0))
            heard(2)
            spread(0, resp, table_a)
            arrived(("U", 0), ("D", 1))
            start(("FU",), ("FD",), ("R", 3, 0), ("L", 1, 1), ("R", 1, 1), ("L", 3, 0))
            arrived(("R", 0, 1), ("L", 0, 0))
        elif s == 3:
            arrived(("FR", 0), ("FL", 0))
            start(("VU",), ("VD",))
            counts[0].wait_recv()
            count_send[1] = count_send[0] + count_recv[0]
            counts[1].start()
            counts[2].start()
        elif s == 4:
            arrived(("U", 1), ("D", 0))
            start(("R", 1, 0), ("L", 3, 1), ("R", 3, 1), ("L", 1, 0))
        elif s == 6:
            arrived(("R", 3, 0), ("L", 1, 1))
            start(("FR", 3), ("FL", 1))
            arrived(("L", 1, 0))
        elif s == 7:
            arrived(("FU",), ("FD",))
            start(("R", 2, 0), ("L", 2, 1), ("R", 2, 1), ("L", 2, 0))
            every(lambda k: spread_copy(0, resp, table_a, k).wait_recv())
            deliver(1, table_a, send_b, partner_kv)
            arrived(("R", 1, 0), ("R", 1, 1))
        elif s == 8:
            arrived(("L", 3, 1), ("L", 3, 0))
            counts[1].wait_recv()
            counts[2].wait_recv()
            counts[3].start()
        elif s == 9:
            arrived(("R", 3, 1))
        elif s == 11:
            arrived(("R", 2, 0), ("L", 2, 1))
            start(("FR", 2), ("FL", 2))
            arrived(("L", 2, 0))
        elif s == 12:
            arrived(("R", 2, 1))
            counts[3].wait_recv()
            count_send[2] = count_send[1] + count_recv[1] + count_recv[2] + count_recv[3]
            counts[4].start()
        elif s == 13:
            arrived(("VU",), ("FR", 3))
        elif s == 14:
            arrived(("VD",), ("FL", 1))
        elif s == 15:
            every(lambda k: deliver_copy(1, send_b, partner_kv, k).wait_recv())
            own_scores()
            arrived(("FR", 2), ("FL", 2))

    def gather_step(s, carry):
        for k in (1, 3, 4, 6, 7, 8, 9, 11, 12, 13, 14, 15):
            @pl.when(s == k)
            def _(k=k):
                gather_events(k)

        slot = slot_at(GATHER_ORDER, s)
        keys, values = kv[slot, :, KEYS], kv[slot, :, VALUES]
        for n in range(ROWS // WIDE):
            tile = pl.ds(n * WIDE, WIDE)
            scores[slot, :, tile] = dot(keys, q_cols[:, tile])
            dprobs[slot, :, tile] = dot(values, w_cols[:, tile])
        take_in(slot)
        return carry

    lax.fori_loop(0, MEMBERS, gather_step, 0)

    for n in range(TILES):
        tile = pl.ds(n * BLK, BLK)
        m = peak[:, tile]
        top = jnp.max(m, axis=0, keepdims=True)
        fade = jnp.exp2((m - top) * c)
        mass = jnp.sum(total[:, tile] * fade, axis=0, keepdims=True)
        delta = jnp.sum(weigh[:, tile] * fade, axis=0, keepdims=True) / mass
        peak[:, tile] = jnp.broadcast_to(top + jnp.log2(mass) * (1.0 / c), (8, BLK))
        weigh[:, tile] = jnp.broadcast_to(delta, (8, BLK))

    def probabilities(slot):
        for n in range(TILES):
            tile = pl.ds(n * BLK, BLK)
            s = scores[slot, :, tile].reshape(CHUNK // 8, 8, BLK)
            d = dprobs[slot, :, tile].reshape(CHUNK // 8, 8, BLK)
            p = jnp.exp2((s - peak[:, tile][None]) * c)
            ds = p * (d - weigh[:, tile][None])
            p_low[:, tile] = p.reshape(CHUNK, BLK).astype(BF16)
            ds_low[:, tile] = ds.reshape(CHUNK, BLK).astype(BF16)

    def add_query_grad(keys, tile):
        dq_cols[:, tile] += lax.dot_general(
            keys, ds_low[:, tile], (((0,), (0,)), ((), ())), preferred_element_type=F32
        )

    def own_grads():
        probabilities(OWN)
        for i in range(NB):
            tile = pl.ds(i * QPK * BLK, QPK * BLK)
            d_keys = dot(ds_low[:, tile], q_rows[tile, :])
            d_values = dot(p_low[:, tile], w_rows[tile, :])
            add_query_grad(own_pair(i, KEYS), tile)
            own_grad[i, :, KEYS] = d_keys[:BLK]
            own_grad[i, :, VALUES] = d_values[:BLK]
            give[i, :, KEYS] = d_keys[BLK:].astype(BF16)
            give[i, :, VALUES] = d_values[BLK:].astype(BF16)
        spread(2, give, table_c)

    def keep(a, b, h):
        g_send[a * SIDE + b, halves[h]] = g_tmp[halves[h]].astype(BF16)

    def join_right(a):
        arrived(("r", a))
        g_send[a * SIDE + 1, UP] = (g_hold[a] + x_rel_a[a // 2].astype(F32)).astype(BF16)
        start(("gr", a, 0))

    def join_left(a):
        arrived(("l", a))
        g_send[a * SIDE + 3, DOWN] = (g_hold[a + 1] + x_rel_b[a // 2].astype(F32)).astype(BF16)
        start(("gl", a, 1))

    def x_combined(a, h):
        arrived(("gr", a, h), ("gl", a, h))
        half = halves[h]
        return x_sum[a, half] + x_in_l[a, half].astype(F32) + x_in_r[a, half].astype(F32)

    def reduce_events(p):
        a, b = REDUCE_ORDER[p]
        if b == 0:
            x_sum[a] = g_tmp[...]
        elif (a, b) == (0, 2):
            arrived(("yu",), ("yd",))
            g_send[2] = (g_tmp[...] + z_far[0].astype(F32) + z_far[1].astype(F32)).astype(BF16)
        elif a % 2 or b == 2:
            keep(a, b, 0)
            keep(a, b, 1)
        elif b == 1:
            keep(a, 1, 1)
            g_hold[a] = g_tmp[UP]
        else:
            keep(a, 3, 0)
            g_hold[a + 1] = g_tmp[DOWN]
        if p == 0:
            start(("r", 2), ("l", 2))
        elif p == 1:
            start(("yd",))
        elif p == 2:
            start(("yu",))
        elif p == 3:
            start(("gr", 2, 1))
        elif p == 4:
            start(("gl", 2, 0))
            join_right(2)
            join_left(2)
        elif p == 5:
            own_grads()
        elif p == 6:
            start(("gr", 1, 1))
        elif p == 7:
            start(("gr", 3, 0), ("gr", 1, 0), ("gr", 3, 1))
        elif p == 8:
            start(("gl", 1, 1))
        elif p == 9:
            start(("gl", 3, 0), ("gl", 1, 0), ("gl", 3, 1))
            for h in range(2):
                z_send[2, halves[h]] = x_combined(2, h).astype(BF16)
            start(("zr",), ("zl",))
        elif p == 12:
            start(("r", 0), ("l", 0))
            z_send[1, DOWN] = x_combined(1, 1).astype(BF16)
            start(("zu", 1))
            z_send[3, UP] = x_combined(3, 0).astype(BF16)
            start(("zd", 0))
        elif p == 13:
            start(("gr", 0, 1))
            every(lambda k: spread_copy(2, give, table_c, k).wait_recv())
            deliver(3, table_c, send_d, partner_grad)
        elif p == 14:
            start(("gl", 0, 0))
            join_right(0)
            join_left(0)
            value = x_combined(1, 0)
            arrived(("zr",))
            z_send[1, UP] = (value + z_rel_a[...].astype(F32)).astype(BF16)
            start(("zu", 0))
            value = x_combined(3, 1)
            arrived(("zl",))
            z_send[3, DOWN] = (value + z_rel_b[...].astype(F32)).astype(BF16)
            start(("zd", 1))

    def reduce_step(p, carry):
        slot = slot_at(REDUCE_ORDER, p)
        probabilities(slot)
        g_tmp[:, KEYS] = dot(ds_low[...], q_rows[...])
        g_tmp[:, VALUES] = dot(p_low[...], w_rows[...])
        for n in range(ROWS // WIDE):
            add_query_grad(kv[slot, :, KEYS], pl.ds(n * WIDE, WIDE))

        for k in range(MEMBERS):
            @pl.when(p == k)
            def _(k=k):
                reduce_events(k)

        return carry

    lax.fori_loop(0, MEMBERS, reduce_step, 0)

    counts[4].wait_recv()
    tokens = (count_send[2] + count_recv[4]).astype(F32)
    factor = (LOSS_SCALE * 16 * RESP * CHUNK) / tokens[0:1]
    for i in range(NB):
        for head in range(QPK):
            rows = pl.ds(i * BLK, BLK)
            grads = dq_cols[:, pl.ds((i * QPK + head) * BLK, BLK)]
            grad_query[rows, pl.ds(head * HD, HD)] = (grads.T * (factor * scale)).astype(BF16)

    every(lambda k: deliver_copy(3, send_d, partner_grad, k).wait_recv())
    stream = own_grad[...] + partner_grad[...].astype(F32)
    grad_stream[:, :, KEYS] = (stream[:, :, :HD] * (factor * scale)[None]).astype(BF16)
    grad_stream[:, :, VALUES] = (stream[:, :, HD:] * factor[None]).astype(BF16)

    for h in range(2):
        own = x_combined(0, h)
        arrived(("zu", h), ("zd", h))
        own = own + z_in_l[halves[h]].astype(F32) + z_in_r[halves[h]].astype(F32)
        grad_prompt[halves[h], KEYS] = (own[:, :HD] * (factor * scale)).astype(BF16)
        grad_prompt[halves[h], VALUES] = (own[:, HD:] * factor).astype(BF16)

    for name in copies:
        copies[name].wait_send()
    every(lambda k: spread_copy(0, resp, table_a, k).wait_send())
    every(lambda k: deliver_copy(1, send_b, partner_kv, k).wait_send())
    every(lambda k: spread_copy(2, give, table_c, k).wait_send())
    every(lambda k: deliver_copy(3, send_d, partner_grad, k).wait_send())
    for cp in counts:
        cp.wait_send()


def local(query, resp_kv, prompt_kv, grad_out, rewards, lengths, block_order):
    vmem = pl.BlockSpec(memory_space=pltpu.VMEM)
    hbm = pl.BlockSpec(memory_space=pl.ANY)
    pair = (CHUNK, 2 * HD)
    half = (BLK, 2 * HD)
    blocks = (NB, BLK, 2 * HD)
    pieces = (NB * MEMBERS, 16, HD)
    wide = (CHUNK, QPK * HD)
    grads = pl.pallas_call(
        kernel,
        name="attention_step",
        out_shape=(
            pltpu.VMEM(wide, BF16),
            pltpu.VMEM(blocks, BF16),
            pltpu.VMEM(pair, BF16),
        ),
        in_specs=[hbm] * 7,
        out_specs=(vmem,) * 3,
        scratch_shapes=[
            pltpu.VMEM(wide, BF16),
            pltpu.VMEM(wide, BF16),
            pltpu.VMEM(blocks, BF16),
            pltpu.SMEM((RESP,), F32),
            pltpu.SMEM((RESP,), jnp.int32),
            pltpu.SMEM((NB * MEMBERS,), jnp.int32),
            pltpu.SMEM((NB * MEMBERS,), jnp.int32),
            pltpu.VMEM((MEMBERS, *pair), BF16),
            pltpu.VMEM((MEMBERS + 1, CHUNK, ROWS), F32),
            pltpu.VMEM((MEMBERS + 1, CHUNK, ROWS), F32),
            pltpu.VMEM((ROWS, HD), BF16),
            pltpu.VMEM((ROWS, HD), BF16),
            pltpu.VMEM((HD, ROWS), BF16),
            pltpu.VMEM((HD, ROWS), BF16),
            pltpu.VMEM((8, ROWS), F32),
            pltpu.VMEM((8, ROWS), F32),
            pltpu.VMEM((8, ROWS), F32),
            pltpu.VMEM((CHUNK, ROWS), BF16),
            pltpu.VMEM((CHUNK, ROWS), BF16),
            pltpu.VMEM((HD, ROWS), F32),
            pltpu.VMEM(pair, F32),
            pltpu.VMEM((MEMBERS, *pair), BF16),
            pltpu.VMEM((4, *half), F32),
            pltpu.VMEM((2, *half), BF16),
            pltpu.VMEM((2, *half), BF16),
            pltpu.VMEM((SIDE, *pair), BF16),
            pltpu.VMEM((SIDE, *pair), BF16),
            pltpu.VMEM((SIDE, *pair), F32),
            pltpu.VMEM((SIDE, *pair), BF16),
            pltpu.VMEM(half, BF16),
            pltpu.VMEM(half, BF16),
            pltpu.VMEM(pair, BF16),
            pltpu.VMEM(pair, BF16),
            pltpu.VMEM((2, *pair), BF16),
            pltpu.VMEM(pieces, BF16),
            pltpu.VMEM(pieces, BF16),
            pltpu.VMEM(blocks, BF16),
            pltpu.VMEM(pieces, BF16),
            pltpu.VMEM(pieces, BF16),
            pltpu.VMEM(blocks, BF16),
            pltpu.VMEM(blocks, BF16),
            pltpu.VMEM(blocks, F32),
            pltpu.VMEM((3, 8, HD), jnp.int32),
            pltpu.VMEM((5, 8, HD), jnp.int32),
            pltpu.SemaphoreType.DMA((N_COPIES,)),
            pltpu.SemaphoreType.DMA((N_COPIES,)),
            pltpu.SemaphoreType.DMA((4, MEMBERS)),
            pltpu.SemaphoreType.DMA((4, MEMBERS)),
            pltpu.SemaphoreType.DMA((5,)),
            pltpu.SemaphoreType.DMA((5,)),
            pltpu.SemaphoreType.DMA((7,)),
            pltpu.SemaphoreType.REGULAR((3,)),
        ],
        compiler_params=pltpu.CompilerParams(
            collective_id=0, has_side_effects=True, vmem_limit_bytes=58 * 2**20
        ),
    )(
        query[0], resp_kv[0].reshape(blocks), prompt_kv[0], grad_out[0],
        rewards[0], lengths[0], block_order[0],
    )
    return grads[0][None], grads[1].reshape(1, *pair), grads[2][None]


def solution(mesh):
    rows = P("grp", "seq", None)
    small = P("grp", None)
    return jax.shard_map(
        local,
        mesh=mesh,
        in_specs=(rows, rows, rows, rows, small, small, small),
        out_specs=(rows, rows, rows),
        check_vma=False,
    )
```

```python
import jax
import jax.numpy as jnp
from jax import lax
from jax.experimental import pallas as pl
from jax.experimental.pallas import tpu as pltpu
from jax.sharding import PartitionSpec as P

RESP = 16
BLK = 128
NB = 2
HD = 128
QPK = 5
LOSS_SCALE = 32.0
NEG = -1e30
LOG2E = 1.4426950408889634
MESH = pl.DeviceIdType.MESH
F32 = jnp.float32
BF16 = jnp.bfloat16

SIDE = 4
MEMBERS = SIDE * SIDE
CHUNK = NB * BLK
ROWS = NB * QPK * BLK
TILES = NB * QPK
WIDE = 256

UP = pl.ds(0, BLK)
DOWN = pl.ds(BLK, BLK)
KEYS = pl.ds(0, HD)
VALUES = pl.ds(HD, HD)
OWN = MEMBERS

GATHER_ORDER = (
    (0, 0), (0, 1), (0, 3), (0, 2), (3, 0), (1, 0), (1, 1), (1, 3),
    (3, 1), (3, 3), (2, 0), (2, 1), (2, 3), (3, 2), (1, 2), (2, 2),
)
REDUCE_ORDER = (
    (2, 2), (3, 2), (1, 2), (2, 1), (2, 3), (2, 0), (1, 1), (3, 1),
    (1, 3), (3, 3), (1, 0), (3, 0), (0, 2), (0, 1), (0, 3), (0, 0),
)
REDUCE_EVENTS = (
    (("far", 2),),
    (("far", 3),),
    (("far", 1),),
    (("gr", 2, 1),),
    (("gl", 2, 0), ("gr", 2, 0), ("gl", 2, 1)),
    (("own",), ("spread",)),
    (("gr", 1, 1),),
    (("gr", 3, 0), ("gr", 1, 0), ("gr", 3, 1)),
    (("gl", 1, 1),),
    (("gl", 3, 0), ("gl", 1, 0), ("gl", 3, 1), ("z", 2, 0), ("z", 2, 1)),
    (),
    (),
    (("far", 0), ("z", 1, 1), ("z", 3, 0), ("deliver",)),
    (("gr", 0, 1),),
    (("gl", 0, 0), ("z", 1, 0), ("z", 3, 1), ("gr", 0, 0), ("gl", 0, 1)),
    (),
)
N_COPIES = 60


def dot(a, b):
    return jnp.dot(a, b, preferred_element_type=F32)


def wrapped(t, n):
    return t - jnp.where(t >= n, n, 0)


def slot_at(sequence, step):
    slot = jnp.int32(0)
    for k, (a, b) in enumerate(sequence):
        slot = slot + jnp.where(step == k, a * SIDE + b, 0)
    return slot


def kernel(
    query_hbm, resp_hbm, prompt_hbm, grad_out_hbm, rewards_hbm, lengths_hbm, order_hbm,
    grad_query, grad_stream, grad_prompt,
    query, grad_out, resp, rewards, lengths, order, partner,
    kv, scores, dprobs, q_rows, w_rows, q_cols, w_cols,
    peak, total, weigh, p_low, ds_low, dq_cols, g_tmp, g_send, g_hold,
    x_rel_a, x_rel_b, x_in_l, x_in_r, x_sum,
    z_send, z_rel, z_in_l, z_in_r, z_far,
    table_a, send_b, partner_kv, table_c, send_d, partner_grad, give, own_grad,
    count_send, count_recv,
    ssem, rsem, esend, erecv, csend, crecv, isem, known,
):
    scale = HD ** (-0.5)
    c = scale * LOG2E
    me = lax.axis_index("seq")
    grp = lax.axis_index("grp")
    z, x = me // SIDE, me % SIDE
    right = z * SIDE + (x + 1) % SIDE
    left = z * SIDE + (x + SIDE - 1) % SIDE
    above = ((z + 1) % SIDE) * SIDE + x
    below = ((z + SIDE - 1) % SIDE) * SIDE + x

    inputs = [
        pltpu.make_async_copy(src, dst, isem.at[k])
        for k, (src, dst) in enumerate((
            (prompt_hbm, kv.at[0]), (resp_hbm, resp), (order_hbm, order), (lengths_hbm, lengths),
            (rewards_hbm, rewards), (query_hbm, query), (grad_out_hbm, grad_out),
        ))
    ]
    for load in inputs:
        load.start()

    copies = {}

    def declare(name, src, dst, dev):
        k = len(copies)
        copies[name] = pltpu.make_async_remote_copy(
            src_ref=src, dst_ref=dst, send_sem=ssem.at[k], recv_sem=rsem.at[k],
            device_id={"seq": dev}, device_id_type=MESH,
        )

    def slot_ref(a, b, half):
        return kv.at[a * SIDE + b, half]

    halves = (UP, DOWN)
    for a in range(SIDE):
        for h in range(2):
            declare(("R", a, h), slot_ref(a, 0, halves[h]), slot_ref(a, 3, halves[h]), right)
            declare(("L", a, h), slot_ref(a, 0, halves[h]), slot_ref(a, 1, halves[h]), left)
            declare(("gr", a, h), g_send.at[a * SIDE + 1, halves[h]], x_in_l.at[a, halves[h]], right)
            declare(("gl", a, h), g_send.at[a * SIDE + 3, halves[h]], x_in_r.at[a, halves[h]], left)
        if a != 1:
            declare(("FR", a), slot_ref(a, 3, UP), slot_ref(a, 2, UP), right)
        if a != 3:
            declare(("FL", a), slot_ref(a, 1, DOWN), slot_ref(a, 2, DOWN), left)
        if a != 1:
            declare(("r", a), g_send.at[a * SIDE + 2, UP], x_rel_a.at[a], right)
        if a != 3:
            declare(("l", a), g_send.at[a * SIDE + 2, DOWN], x_rel_b.at[a], left)
    for h in range(2):
        declare(("U", h), slot_ref(0, 0, halves[h]), slot_ref(3, 0, halves[h]), above)
        declare(("D", h), slot_ref(0, 0, halves[h]), slot_ref(1, 0, halves[h]), below)
        declare(("zu", h), z_send.at[1, halves[h]], z_in_l.at[halves[h]], above)
        declare(("zd", h), z_send.at[3, halves[h]], z_in_r.at[halves[h]], below)
    declare(("VU",), slot_ref(0, 2, DOWN), slot_ref(3, 2, DOWN), above)
    declare(("VD",), slot_ref(0, 2, UP), slot_ref(1, 2, UP), below)
    declare(("yu",), g_send.at[SIDE + 2, UP], z_far.at[UP], above)
    declare(("yd",), g_send.at[3 * SIDE + 2, DOWN], z_far.at[DOWN], below)
    declare(("FU",), slot_ref(3, 0, UP), slot_ref(2, 0, UP), above)
    declare(("FD",), slot_ref(1, 0, DOWN), slot_ref(2, 0, DOWN), below)
    declare(("zr",), z_send.at[2, UP], z_rel.at[UP], above)
    declare(("zl",), z_send.at[2, DOWN], z_rel.at[DOWN], below)

    def start(*names):
        for name in names:
            copies[name].start()

    def arrived(*names):
        for name in names:
            copies[name].wait_recv()

    def piece(t):
        second = jnp.where(t >= MEMBERS // 2, 1, 0)
        return (
            slice(None),
            pl.ds(pl.multiple_of((t - second * (MEMBERS // 2)) * 16, 16), 16),
            pl.ds(pl.multiple_of(second * HD, HD), HD),
        )

    def spread_copy(stage, src, dst, k):
        t = wrapped(me + k, MEMBERS)
        return pltpu.make_async_remote_copy(
            src_ref=src.at[piece(t)], dst_ref=dst.at[pl.ds(NB * k, NB)],
            send_sem=esend.at[stage, k], recv_sem=erecv.at[stage, k],
            device_id={"seq": t}, device_id_type=MESH,
        )

    def deliver_copy(stage, src, dst, k):
        t = wrapped(me + k, MEMBERS)
        return pltpu.make_async_remote_copy(
            src_ref=src.at[pl.ds(NB * k, NB)], dst_ref=dst.at[piece(me)],
            send_sem=esend.at[stage, k], recv_sem=erecv.at[stage, k],
            device_id={"seq": t}, device_id_type=MESH,
        )

    def every(fn):
        def body(k, carry):
            fn(k)
            return carry

        lax.fori_loop(1, MEMBERS, body, 0)

    def spread(stage, src, dst):
        every(lambda k: spread_copy(stage, src, dst, k).start())
        dst[pl.ds(0, NB)] = src[piece(me)]

    def deliver(stage, table, buf, dst):
        def fill(k, carry):
            for i in range(NB):
                buf[NB * k + i] = table[partner[NB * wrapped(me + k, MEMBERS) + i]]
            return carry

        lax.fori_loop(0, MEMBERS, fill, 0)
        every(lambda k: deliver_copy(stage, buf, dst, k).start())
        dst[piece(me)] = buf[pl.ds(0, NB)]

    def find_partners():
        def one(j, carry):
            b = order[j]
            sibling = b + 1 - 2 * lax.rem(b, NB)
            found = jnp.int32(0)
            for k in range(MEMBERS):
                far = wrapped(me + MEMBERS - k, MEMBERS) * NB
                for i in range(NB):
                    found = found + jnp.where(order[NB * k + i] == sibling, far + i, 0)
            partner[j] = found
            return carry

        lax.fori_loop(0, NB * MEMBERS, one, 0)

    mate = grp + 1 - 2 * (grp % 2)
    y_next = (grp // 8) * 8 + (grp % 8 + 2) % 8
    y_last = (grp // 8) * 8 + (grp % 8 + 6) % 8
    z_mate = (grp + 8) % 16
    counts = [
        pltpu.make_async_remote_copy(
            src_ref=src, dst_ref=count_recv.at[k], send_sem=csend.at[k], recv_sem=crecv.at[k],
            device_id={"grp": peer}, device_id_type=MESH,
        )
        for k, (src, peer) in enumerate((
            (count_send.at[0], mate), (count_send.at[1], y_next), (count_send.at[1], y_last),
            (count_recv.at[1], y_next), (count_send.at[2], z_mate),
        ))
    ]

    neighbours = (right, left, above, below)
    barrier = pltpu.get_barrier_semaphore()
    for dev in neighbours:
        pl.semaphore_signal(barrier, inc=1, device_id={"seq": dev}, device_id_type=MESH)
    for dev in (mate, y_next, y_last, z_mate):
        pl.semaphore_signal(barrier, inc=1, device_id={"grp": dev}, device_id_type=MESH)

    def pass_on(k):
        for dev in neighbours:
            pl.semaphore_signal(known.at[k], inc=1, device_id={"seq": dev}, device_id_type=MESH)

    def heard(k):
        pl.semaphore_wait(known.at[k], len(neighbours))

    inputs[0].wait()
    pl.semaphore_wait(barrier, 8)

    start(("U", 0), ("D", 1), ("R", 0, 0), ("L", 0, 1), ("U", 1), ("D", 0), ("R", 0, 1), ("L", 0, 0))
    pass_on(0)
    for load in inputs[1:]:
        load.wait()
    tokens = lengths[0]
    for r in range(1, RESP):
        tokens = tokens + lengths[r]
    count_send[0] = jnp.full((8, HD), tokens, jnp.int32)
    counts[0].start()
    heard(0)
    pass_on(1)

    mean = rewards[0]
    for r in range(1, RESP):
        mean = mean + rewards[r]
    mean = mean * (1.0 / RESP)
    is_later = []
    row_number = lax.broadcasted_iota(jnp.int32, (BLK, HD), 0)
    for i in range(NB):
        b = order[NB * me + i]
        r, h = b // NB, b % NB
        is_later.append(h)
        gain = jnp.where(row_number + h * BLK < lengths[r], rewards[r] - mean, 0.0)
        for head in range(QPK):
            tile = pl.ds((i * QPK + head) * BLK, BLK)
            rows = pl.ds(i * BLK, BLK)
            cols = pl.ds(head * HD, HD)
            q = query[rows, cols].astype(F32)
            w = grad_out[rows, cols].astype(F32) * gain
            q_rows[tile, :] = q.astype(BF16)
            w_rows[tile, :] = w.astype(BF16)
            q_cols[:, tile] = q.T.astype(BF16)
            w_cols[:, tile] = w.T.astype(BF16)
    heard(1)
    pass_on(2)
    find_partners()
    peak[...] = jnp.full_like(peak, NEG)
    total[...] = jnp.zeros_like(total)
    weigh[...] = jnp.zeros_like(weigh)
    dq_cols[...] = jnp.zeros_like(dq_cols)

    def take_in(slot, tiles=range(TILES)):
        for n in tiles:
            tile = pl.ds(n * BLK, BLK)
            s = scores[slot, :, tile].reshape(CHUNK // 8, 8, BLK)
            d = dprobs[slot, :, tile].reshape(CHUNK // 8, 8, BLK)
            before = peak[:, tile]
            now = jnp.maximum(before, jnp.max(s, axis=0))
            fade = jnp.exp2((before - now) * c)
            e = jnp.exp2((s - now[None]) * c)
            total[:, tile] = total[:, tile] * fade + jnp.sum(e, axis=0)
            weigh[:, tile] = weigh[:, tile] * fade + jnp.sum(e * d, axis=0)
            peak[:, tile] = now

    def own_pair(i, cols):
        return jnp.concatenate([resp[i, :, cols], partner_kv[i, :, cols]], axis=0)

    def own_scores():
        key = lax.broadcasted_iota(jnp.int32, (CHUNK, BLK), 0)
        pos = lax.broadcasted_iota(jnp.int32, (CHUNK, BLK), 1)
        for i in range(NB):
            limit = jnp.where(is_later[i] == 1, CHUNK, BLK)
            seen = jnp.where(key < BLK, pos - key, limit - 1 - key) >= 0
            k_own, v_own = own_pair(i, KEYS), own_pair(i, VALUES)
            for head in range(QPK):
                tile = pl.ds((i * QPK + head) * BLK, BLK)
                scores[OWN, :, tile] = jnp.where(seen, dot(k_own, q_cols[:, tile]), NEG)
                dprobs[OWN, :, tile] = dot(v_own, w_cols[:, tile])
        take_in(OWN)

    def gather_events(s):
        if s == 1:
            arrived(("R", 0, 0), ("L", 0, 1))
            start(("FR", 0), ("FL", 0))
            heard(2)
            spread(0, resp, table_a)
            arrived(("U", 0), ("D", 1))
            start(("FU",), ("FD",), ("R", 3, 0), ("L", 1, 1), ("R", 1, 1), ("L", 3, 0))
            arrived(("R", 0, 1), ("L", 0, 0))
        elif s == 3:
            arrived(("FR", 0), ("FL", 0))
            start(("VU",), ("VD",))
            counts[0].wait_recv()
            count_send[1] = count_send[0] + count_recv[0]
            counts[1].start()
            counts[2].start()
        elif s == 4:
            arrived(("U", 1), ("D", 0))
            start(("R", 1, 0), ("L", 3, 1), ("R", 3, 1), ("L", 1, 0))
        elif s == 6:
            arrived(("R", 3, 0), ("L", 1, 1))
            start(("FR", 3), ("FL", 1))
            arrived(("L", 1, 0))
        elif s == 7:
            arrived(("FU",), ("FD",))
            start(("R", 2, 0), ("L", 2, 1), ("R", 2, 1), ("L", 2, 0))
            every(lambda k: spread_copy(0, resp, table_a, k).wait_recv())
            deliver(1, table_a, send_b, partner_kv)
            arrived(("R", 1, 0), ("R", 1, 1))
        elif s == 8:
            arrived(("L", 3, 1), ("L", 3, 0))
            counts[1].wait_recv()
            counts[2].wait_recv()
            counts[3].start()
        elif s == 9:
            arrived(("R", 3, 1))
        elif s == 11:
            arrived(("R", 2, 0), ("L", 2, 1))
            start(("FR", 2), ("FL", 2))
            arrived(("L", 2, 0))
        elif s == 12:
            arrived(("R", 2, 1))
            counts[3].wait_recv()
            count_send[2] = count_send[1] + count_recv[1] + count_recv[2] + count_recv[3]
            counts[4].start()
        elif s == 13:
            arrived(("VU",), ("FR", 3))
        elif s == 14:
            arrived(("VD",), ("FL", 1))
        elif s == 15:
            every(lambda k: deliver_copy(1, send_b, partner_kv, k).wait_recv())
            own_scores()
            arrived(("FR", 2), ("FL", 2))

    def gather_step(s, carry):
        for k in (1, 3, 4, 6, 7, 8, 9, 11, 12, 13, 14, 15):
            @pl.when(s == k)
            def _(k=k):
                gather_events(k)

        slot = slot_at(GATHER_ORDER, s)
        keys, values = kv[slot, :, KEYS], kv[slot, :, VALUES]
        for n in range(ROWS // WIDE):
            tile = pl.ds(n * WIDE, WIDE)
            scores[slot, :, tile] = dot(keys, q_cols[:, tile])
            dprobs[slot, :, tile] = dot(values, w_cols[:, tile])
            if n:
                take_in(slot, (2 * n - 2, 2 * n - 1))
        take_in(slot, (TILES - 2, TILES - 1))
        return carry

    lax.fori_loop(0, MEMBERS, gather_step, 0)

    for n in range(TILES):
        tile = pl.ds(n * BLK, BLK)
        m = peak[:, tile]
        top = jnp.max(m, axis=0, keepdims=True)
        fade = jnp.exp2((m - top) * c)
        mass = jnp.sum(total[:, tile] * fade, axis=0, keepdims=True)
        delta = jnp.sum(weigh[:, tile] * fade, axis=0, keepdims=True) / mass
        peak[:, tile] = jnp.broadcast_to(top + jnp.log2(mass) * (1.0 / c), (8, BLK))
        weigh[:, tile] = jnp.broadcast_to(delta, (8, BLK))

    def probabilities(slot, tiles=range(TILES)):
        for n in tiles:
            tile = pl.ds(n * BLK, BLK)
            s = scores[slot, :, tile].reshape(CHUNK // 8, 8, BLK)
            d = dprobs[slot, :, tile].reshape(CHUNK // 8, 8, BLK)
            p = jnp.exp2((s - peak[:, tile][None]) * c)
            ds = p * (d - weigh[:, tile][None])
            p_low[:, tile] = p.reshape(CHUNK, BLK).astype(BF16)
            ds_low[:, tile] = ds.reshape(CHUNK, BLK).astype(BF16)

    def add_query_grad(keys, tile):
        dq_cols[:, tile] += lax.dot_general(
            keys, ds_low[:, tile], (((0,), (0,)), ((), ())), preferred_element_type=F32
        )

    def own_grads():
        probabilities(OWN)
        for i in range(NB):
            tile = pl.ds(i * QPK * BLK, QPK * BLK)
            d_keys = dot(ds_low[:, tile], q_rows[tile, :])
            d_values = dot(p_low[:, tile], w_rows[tile, :])
            add_query_grad(own_pair(i, KEYS), tile)
            own_grad[i, :, KEYS] = d_keys[:BLK]
            own_grad[i, :, VALUES] = d_values[:BLK]
            give[i, :, KEYS] = d_keys[BLK:].astype(BF16)
            give[i, :, VALUES] = d_values[BLK:].astype(BF16)

    def joins(a, b, h):
        return (b == 1 and h == 0 and a != 1) or (b == 3 and h == 1 and a != 3)

    def put_by(a, b):
        if b == 0:
            x_sum[a] = g_tmp[...]
        elif (a, b) != (0, 2):
            for h in range(2):
                if joins(a, b, h):
                    g_hold[2 * a + b // 2] = g_tmp[halves[h]]
                else:
                    g_send[a * SIDE + b, halves[h]] = g_tmp[halves[h]].astype(BF16)

    def x_combined(a, h):
        arrived(("gr", a, h), ("gl", a, h))
        half = halves[h]
        return x_sum[a, half] + x_in_l[a, half].astype(F32) + x_in_r[a, half].astype(F32)

    def reduce_event(kind, a=0, h=0):
        half = halves[h]
        if kind == "far":
            if a == 0:
                arrived(("yu",), ("yd",))
                g_send[2] = (g_tmp[...] + z_far[...].astype(F32)).astype(BF16)
            start(("yu",) if a == 1 else ("r", a), ("yd",) if a == 3 else ("l", a))
        elif kind in ("gr", "gl"):
            b, relay, landed = (1, "r", x_rel_a) if kind == "gr" else (3, "l", x_rel_b)
            if joins(a, b, h):
                arrived((relay, a))
                g_send[a * SIDE + b, half] = (g_hold[2 * a + b // 2] + landed[a].astype(F32)).astype(BF16)
            start((kind, a, h))
        elif kind == "z":
            value = x_combined(a, h)
            if (a, h) == (1, 0):
                arrived(("zr",))
                value = value + z_rel[half].astype(F32)
            elif (a, h) == (3, 1):
                arrived(("zl",))
                value = value + z_rel[half].astype(F32)
            z_send[a, half] = value.astype(BF16)
            start({1: ("zu", h), 2: ("zr",) if h == 0 else ("zl",), 3: ("zd", h)}[a])
        elif kind == "own":
            own_grads()
        elif kind == "spread":
            spread(2, give, table_c)
        else:
            every(lambda k: spread_copy(2, give, table_c, k).wait_recv())
            deliver(3, table_c, send_d, partner_grad)

    def reduce_step(p, carry):
        slot = slot_at(REDUCE_ORDER, p)
        keys = kv[slot, :, KEYS]
        d_keys = jnp.zeros((CHUNK, HD), F32)
        d_values = jnp.zeros((CHUNK, HD), F32)
        for n in range(ROWS // WIDE):
            tile = pl.ds(n * WIDE, WIDE)
            probabilities(slot, (2 * n, 2 * n + 1))
            d_keys = d_keys + dot(ds_low[:, tile], q_rows[tile, :])
            d_values = d_values + dot(p_low[:, tile], w_rows[tile, :])
            add_query_grad(keys, tile)
        g_tmp[:, KEYS] = d_keys
        g_tmp[:, VALUES] = d_values

        for k in range(MEMBERS):
            @pl.when(p == k)
            def _(k=k):
                put_by(*REDUCE_ORDER[k])
                for event in REDUCE_EVENTS[k]:
                    reduce_event(*event)

        return carry

    lax.fori_loop(0, MEMBERS, reduce_step, 0)

    counts[4].wait_recv()
    tokens = (count_send[2] + count_recv[4]).astype(F32)
    factor = (LOSS_SCALE * 16 * RESP * CHUNK) / tokens[0:1]
    for i in range(NB):
        for head in range(QPK):
            rows = pl.ds(i * BLK, BLK)
            grads = dq_cols[:, pl.ds((i * QPK + head) * BLK, BLK)]
            grad_query[rows, pl.ds(head * HD, HD)] = (grads.T * (factor * scale)).astype(BF16)

    every(lambda k: deliver_copy(3, send_d, partner_grad, k).wait_recv())
    stream = own_grad[...] + partner_grad[...].astype(F32)
    grad_stream[:, :, KEYS] = (stream[:, :, :HD] * (factor * scale)[None]).astype(BF16)
    grad_stream[:, :, VALUES] = (stream[:, :, HD:] * factor[None]).astype(BF16)

    for h in range(2):
        own = x_combined(0, h)
        arrived(("zu", h), ("zd", h))
        own = own + z_in_l[halves[h]].astype(F32) + z_in_r[halves[h]].astype(F32)
        grad_prompt[halves[h], KEYS] = (own[:, :HD] * (factor * scale)).astype(BF16)
        grad_prompt[halves[h], VALUES] = (own[:, HD:] * factor).astype(BF16)

    for name in copies:
        copies[name].wait_send()
    every(lambda k: spread_copy(0, resp, table_a, k).wait_send())
    every(lambda k: deliver_copy(1, send_b, partner_kv, k).wait_send())
    every(lambda k: spread_copy(2, give, table_c, k).wait_send())
    every(lambda k: deliver_copy(3, send_d, partner_grad, k).wait_send())
    for cp in counts:
        cp.wait_send()


def write_out(query, stream, prompt, query_out, stream_out, prompt_out, sem):
    copies = [
        pltpu.make_async_copy(src, dst, sem.at[k])
        for k, (src, dst) in enumerate(((query, query_out), (stream, stream_out), (prompt, prompt_out)))
    ]
    for cp in copies:
        cp.start()
    for cp in copies:
        cp.wait()


def local(query, resp_kv, prompt_kv, grad_out, rewards, lengths, block_order):
    vmem = pl.BlockSpec(memory_space=pltpu.VMEM)
    hbm = pl.BlockSpec(memory_space=pl.ANY)
    pair = (CHUNK, 2 * HD)
    half = (BLK, 2 * HD)
    blocks = (NB, BLK, 2 * HD)
    pieces = (NB * MEMBERS, 16, HD)
    wide = (CHUNK, QPK * HD)
    grads = pl.pallas_call(
        kernel,
        name="attention_step",
        out_shape=(
            pltpu.VMEM(wide, BF16),
            pltpu.VMEM(blocks, BF16),
            pltpu.VMEM(pair, BF16),
        ),
        in_specs=[hbm] * 7,
        out_specs=(vmem,) * 3,
        scratch_shapes=[
            pltpu.VMEM(wide, BF16),
            pltpu.VMEM(wide, BF16),
            pltpu.VMEM(blocks, BF16),
            pltpu.SMEM((RESP,), F32),
            pltpu.SMEM((RESP,), jnp.int32),
            pltpu.SMEM((NB * MEMBERS,), jnp.int32),
            pltpu.SMEM((NB * MEMBERS,), jnp.int32),
            pltpu.VMEM((MEMBERS, *pair), BF16),
            pltpu.VMEM((MEMBERS + 1, CHUNK, ROWS), F32),
            pltpu.VMEM((MEMBERS + 1, CHUNK, ROWS), F32),
            pltpu.VMEM((ROWS, HD), BF16),
            pltpu.VMEM((ROWS, HD), BF16),
            pltpu.VMEM((HD, ROWS), BF16),
            pltpu.VMEM((HD, ROWS), BF16),
            pltpu.VMEM((8, ROWS), F32),
            pltpu.VMEM((8, ROWS), F32),
            pltpu.VMEM((8, ROWS), F32),
            pltpu.VMEM((CHUNK, ROWS), BF16),
            pltpu.VMEM((CHUNK, ROWS), BF16),
            pltpu.VMEM((HD, ROWS), F32),
            pltpu.VMEM(pair, F32),
            pltpu.VMEM((MEMBERS, *pair), BF16),
            pltpu.VMEM((2 * SIDE, *half), F32),
            pltpu.VMEM((SIDE, *half), BF16),
            pltpu.VMEM((SIDE, *half), BF16),
            pltpu.VMEM((SIDE, *pair), BF16),
            pltpu.VMEM((SIDE, *pair), BF16),
            pltpu.VMEM((SIDE, *pair), F32),
            pltpu.VMEM((SIDE, *pair), BF16),
            pltpu.VMEM(pair, BF16),
            pltpu.VMEM(pair, BF16),
            pltpu.VMEM(pair, BF16),
            pltpu.VMEM(pair, BF16),
            pltpu.VMEM(pieces, BF16),
            pltpu.VMEM(pieces, BF16),
            pltpu.VMEM(blocks, BF16),
            pltpu.VMEM(pieces, BF16),
            pltpu.VMEM(pieces, BF16),
            pltpu.VMEM(blocks, BF16),
            pltpu.VMEM(blocks, BF16),
            pltpu.VMEM(blocks, F32),
            pltpu.VMEM((3, 8, HD), jnp.int32),
            pltpu.VMEM((5, 8, HD), jnp.int32),
            pltpu.SemaphoreType.DMA((N_COPIES,)),
            pltpu.SemaphoreType.DMA((N_COPIES,)),
            pltpu.SemaphoreType.DMA((4, MEMBERS)),
            pltpu.SemaphoreType.DMA((4, MEMBERS)),
            pltpu.SemaphoreType.DMA((5,)),
            pltpu.SemaphoreType.DMA((5,)),
            pltpu.SemaphoreType.DMA((7,)),
            pltpu.SemaphoreType.REGULAR((3,)),
        ],
        compiler_params=pltpu.CompilerParams(
            collective_id=0, has_side_effects=True, vmem_limit_bytes=58 * 2**20
        ),
    )(
        query[0], resp_kv[0].reshape(blocks), prompt_kv[0], grad_out[0],
        rewards[0], lengths[0], block_order[0],
    )
    outs = pl.pallas_call(
        write_out,
        name="write_out",
        out_shape=(
            jax.ShapeDtypeStruct(wide, BF16),
            jax.ShapeDtypeStruct(blocks, BF16),
            jax.ShapeDtypeStruct(pair, BF16),
        ),
        in_specs=[vmem] * 3,
        out_specs=(hbm,) * 3,
        scratch_shapes=[pltpu.SemaphoreType.DMA((3,))],
        compiler_params=pltpu.CompilerParams(vmem_limit_bytes=2**20),
    )(*grads)
    return outs[0][None], outs[1].reshape(1, *pair), outs[2][None]


def solution(mesh):
    rows = P("grp", "seq", None)
    small = P("grp", None)
    return jax.shard_map(
        local,
        mesh=mesh,
        in_specs=(rows, rows, rows, rows, small, small, small),
        out_specs=(rows, rows, rows),
        check_vma=False,
    )
```

```python
import jax
import jax.numpy as jnp
from jax import lax
from jax.experimental import pallas as pl
from jax.experimental.pallas import tpu as pltpu
from jax.sharding import PartitionSpec as P

RESP = 16
BLK = 128
NB = 2
HD = 128
QPK = 5
LOSS_SCALE = 32.0
NEG = -1e30
LOG2E = 1.4426950408889634
MESH = pl.DeviceIdType.MESH
F32 = jnp.float32
BF16 = jnp.bfloat16

SIDE = 4
MEMBERS = SIDE * SIDE
CHUNK = NB * BLK
ROWS = NB * QPK * BLK
TILES = NB * QPK
WIDE = 256

UP = pl.ds(0, BLK)
DOWN = pl.ds(BLK, BLK)
KEYS = pl.ds(0, HD)
VALUES = pl.ds(HD, HD)
OWN = MEMBERS

GATHER_ORDER = (
    (0, 0), (0, 1), (0, 3), (0, 2), (3, 0), (1, 0), (1, 1), (1, 3),
    (3, 1), (3, 3), (2, 0), (2, 1), (2, 3), (3, 2), (1, 2), (2, 2),
)
REDUCE_ORDER = (
    (2, 2), (3, 2), (1, 2), (2, 1), (2, 3), (2, 0), (1, 1), (3, 1),
    (1, 3), (3, 3), (1, 0), (3, 0), (0, 2), (0, 1), (0, 3), (0, 0),
)
REDUCE_EVENTS = (
    (("far", 2),),
    (("far", 3), ("own",), ("spread",)),
    (("far", 1),),
    (("gr", 2, 1),),
    (("gl", 2, 0), ("gr", 2, 0), ("gl", 2, 1)),
    (),
    (("gr", 1, 1),),
    (("gr", 3, 0), ("gr", 1, 0), ("gr", 3, 1)),
    (("gl", 1, 1),),
    (("gl", 3, 0), ("gl", 1, 0), ("gl", 3, 1), ("z", 2, 0), ("z", 2, 1)),
    (("deliver",),),
    (),
    (("far", 0), ("z", 1, 1), ("z", 3, 0)),
    (("gr", 0, 1),),
    (("gl", 0, 0), ("z", 1, 0), ("z", 3, 1), ("gr", 0, 0), ("gl", 0, 1)),
    (),
)
N_COPIES = 60


def dot(a, b):
    return jnp.dot(a, b, preferred_element_type=F32)


def wrapped(t, n):
    return t - jnp.where(t >= n, n, 0)


def slot_at(sequence, step):
    slot = jnp.int32(0)
    for k, (a, b) in enumerate(sequence):
        slot = slot + jnp.where(step == k, a * SIDE + b, 0)
    return slot


def kernel(
    query_hbm, resp_hbm, prompt_hbm, grad_out_hbm, rewards_hbm, lengths_hbm, order_hbm,
    grad_query, grad_stream, grad_prompt,
    query, grad_out, resp, rewards, lengths, order, partner,
    kv, scores, dprobs, q_rows, w_rows, q_cols, w_cols,
    peak, total, weigh, p_low, ds_low, dq_cols, g_tmp, g_send, g_hold,
    x_rel_a, x_rel_b, x_in_l, x_in_r, x_sum,
    z_send, z_rel, z_in_l, z_in_r, z_far,
    table_a, send_b, partner_kv, table_c, send_d, partner_grad, give, own_grad,
    count_send, count_recv,
    ssem, rsem, esend, erecv, csend, crecv, isem, known,
):
    scale = HD ** (-0.5)
    c = scale * LOG2E
    me = lax.axis_index("seq")
    grp = lax.axis_index("grp")
    z, x = me // SIDE, me % SIDE
    right = z * SIDE + (x + 1) % SIDE
    left = z * SIDE + (x + SIDE - 1) % SIDE
    above = ((z + 1) % SIDE) * SIDE + x
    below = ((z + SIDE - 1) % SIDE) * SIDE + x

    inputs = [
        pltpu.make_async_copy(src, dst, isem.at[k])
        for k, (src, dst) in enumerate((
            (prompt_hbm, kv.at[0]), (resp_hbm, resp), (order_hbm, order), (lengths_hbm, lengths),
            (rewards_hbm, rewards), (query_hbm, query), (grad_out_hbm, grad_out),
        ))
    ]
    for load in inputs:
        load.start()

    copies = {}

    def declare(name, src, dst, dev):
        k = len(copies)
        copies[name] = pltpu.make_async_remote_copy(
            src_ref=src, dst_ref=dst, send_sem=ssem.at[k], recv_sem=rsem.at[k],
            device_id={"seq": dev}, device_id_type=MESH,
        )

    def slot_ref(a, b, half):
        return kv.at[a * SIDE + b, half]

    halves = (UP, DOWN)
    for a in range(SIDE):
        for h in range(2):
            declare(("R", a, h), slot_ref(a, 0, halves[h]), slot_ref(a, 3, halves[h]), right)
            declare(("L", a, h), slot_ref(a, 0, halves[h]), slot_ref(a, 1, halves[h]), left)
            declare(("gr", a, h), g_send.at[a * SIDE + 1, halves[h]], x_in_l.at[a, halves[h]], right)
            declare(("gl", a, h), g_send.at[a * SIDE + 3, halves[h]], x_in_r.at[a, halves[h]], left)
        if a != 1:
            declare(("FR", a), slot_ref(a, 3, UP), slot_ref(a, 2, UP), right)
        if a != 3:
            declare(("FL", a), slot_ref(a, 1, DOWN), slot_ref(a, 2, DOWN), left)
        if a != 1:
            declare(("r", a), g_send.at[a * SIDE + 2, UP], x_rel_a.at[a], right)
        if a != 3:
            declare(("l", a), g_send.at[a * SIDE + 2, DOWN], x_rel_b.at[a], left)
    for h in range(2):
        declare(("U", h), slot_ref(0, 0, halves[h]), slot_ref(3, 0, halves[h]), above)
        declare(("D", h), slot_ref(0, 0, halves[h]), slot_ref(1, 0, halves[h]), below)
        declare(("zu", h), z_send.at[1, halves[h]], z_in_l.at[halves[h]], above)
        declare(("zd", h), z_send.at[3, halves[h]], z_in_r.at[halves[h]], below)
    declare(("VU",), slot_ref(0, 2, DOWN), slot_ref(3, 2, DOWN), above)
    declare(("VD",), slot_ref(0, 2, UP), slot_ref(1, 2, UP), below)
    declare(("yu",), g_send.at[SIDE + 2, UP], z_far.at[UP], above)
    declare(("yd",), g_send.at[3 * SIDE + 2, DOWN], z_far.at[DOWN], below)
    declare(("FU",), slot_ref(3, 0, UP), slot_ref(2, 0, UP), above)
    declare(("FD",), slot_ref(1, 0, DOWN), slot_ref(2, 0, DOWN), below)
    declare(("zr",), z_send.at[2, UP], z_rel.at[UP], above)
    declare(("zl",), z_send.at[2, DOWN], z_rel.at[DOWN], below)

    def start(*names):
        for name in names:
            copies[name].start()

    def arrived(*names):
        for name in names:
            copies[name].wait_recv()

    def piece(t):
        second = jnp.where(t >= MEMBERS // 2, 1, 0)
        return (
            slice(None),
            pl.ds(pl.multiple_of((t - second * (MEMBERS // 2)) * 16, 16), 16),
            pl.ds(pl.multiple_of(second * HD, HD), HD),
        )

    def spread_copy(stage, src, dst, k):
        t = wrapped(me + k, MEMBERS)
        return pltpu.make_async_remote_copy(
            src_ref=src.at[piece(t)], dst_ref=dst.at[pl.ds(NB * k, NB)],
            send_sem=esend.at[stage, k], recv_sem=erecv.at[stage, k],
            device_id={"seq": t}, device_id_type=MESH,
        )

    def deliver_copy(stage, src, dst, k):
        t = wrapped(me + k, MEMBERS)
        return pltpu.make_async_remote_copy(
            src_ref=src.at[pl.ds(NB * k, NB)], dst_ref=dst.at[piece(me)],
            send_sem=esend.at[stage, k], recv_sem=erecv.at[stage, k],
            device_id={"seq": t}, device_id_type=MESH,
        )

    def every(fn):
        def body(k, carry):
            fn(k)
            return carry

        lax.fori_loop(1, MEMBERS, body, 0)

    def spread(stage, src, dst):
        every(lambda k: spread_copy(stage, src, dst, k).start())
        dst[pl.ds(0, NB)] = src[piece(me)]

    def deliver(stage, table, buf, dst):
        def fill(k, carry):
            for i in range(NB):
                buf[NB * k + i] = table[partner[NB * wrapped(me + k, MEMBERS) + i]]
            return carry

        lax.fori_loop(0, MEMBERS, fill, 0)
        every(lambda k: deliver_copy(stage, buf, dst, k).start())
        dst[piece(me)] = buf[pl.ds(0, NB)]

    def find_partners():
        def one(j, carry):
            b = order[j]
            sibling = b + 1 - 2 * lax.rem(b, NB)
            found = jnp.int32(0)
            for k in range(MEMBERS):
                far = wrapped(me + MEMBERS - k, MEMBERS) * NB
                for i in range(NB):
                    found = found + jnp.where(order[NB * k + i] == sibling, far + i, 0)
            partner[j] = found
            return carry

        lax.fori_loop(0, NB * MEMBERS, one, 0)

    mate = grp + 1 - 2 * (grp % 2)
    y_next = (grp // 8) * 8 + (grp % 8 + 2) % 8
    y_last = (grp // 8) * 8 + (grp % 8 + 6) % 8
    z_mate = (grp + 8) % 16
    counts = [
        pltpu.make_async_remote_copy(
            src_ref=src, dst_ref=count_recv.at[k], send_sem=csend.at[k], recv_sem=crecv.at[k],
            device_id={"grp": peer}, device_id_type=MESH,
        )
        for k, (src, peer) in enumerate((
            (count_send.at[0], mate), (count_send.at[1], y_next), (count_send.at[1], y_last),
            (count_recv.at[1], y_next), (count_send.at[2], z_mate),
        ))
    ]

    neighbours = (right, left, above, below)
    barrier = pltpu.get_barrier_semaphore()
    for dev in neighbours:
        pl.semaphore_signal(barrier, inc=1, device_id={"seq": dev}, device_id_type=MESH)
    for dev in (mate, y_next, y_last, z_mate):
        pl.semaphore_signal(barrier, inc=1, device_id={"grp": dev}, device_id_type=MESH)

    def pass_on(k):
        for dev in neighbours:
            pl.semaphore_signal(known.at[k], inc=1, device_id={"seq": dev}, device_id_type=MESH)

    def heard(k):
        pl.semaphore_wait(known.at[k], len(neighbours))

    inputs[0].wait()
    pl.semaphore_wait(barrier, 8)

    start(("U", 0), ("D", 1), ("R", 0, 0), ("L", 0, 1), ("U", 1), ("D", 0), ("R", 0, 1), ("L", 0, 0))
    pass_on(0)
    for load in inputs[1:]:
        load.wait()
    tokens = lengths[0]
    for r in range(1, RESP):
        tokens = tokens + lengths[r]
    count_send[0] = jnp.full((8, HD), tokens, jnp.int32)
    counts[0].start()
    heard(0)
    pass_on(1)

    mean = rewards[0]
    for r in range(1, RESP):
        mean = mean + rewards[r]
    mean = mean * (1.0 / RESP)
    is_later = []
    row_number = lax.broadcasted_iota(jnp.int32, (BLK, HD), 0)
    for i in range(NB):
        b = order[NB * me + i]
        r, h = b // NB, b % NB
        is_later.append(h)
        gain = jnp.where(row_number + h * BLK < lengths[r], rewards[r] - mean, 0.0)
        for head in range(QPK):
            tile = pl.ds((i * QPK + head) * BLK, BLK)
            rows = pl.ds(i * BLK, BLK)
            cols = pl.ds(head * HD, HD)
            q = query[rows, cols].astype(F32)
            w = grad_out[rows, cols].astype(F32) * gain
            q_rows[tile, :] = q.astype(BF16)
            w_rows[tile, :] = w.astype(BF16)
            q_cols[:, tile] = q.T.astype(BF16)
            w_cols[:, tile] = w.T.astype(BF16)
    heard(1)
    pass_on(2)
    find_partners()
    peak[...] = jnp.full_like(peak, NEG)
    total[...] = jnp.zeros_like(total)
    weigh[...] = jnp.zeros_like(weigh)
    dq_cols[...] = jnp.zeros_like(dq_cols)

    def take_in(slot, tiles=range(TILES)):
        for n in tiles:
            tile = pl.ds(n * BLK, BLK)
            s = scores[slot, :, tile].reshape(CHUNK // 8, 8, BLK)
            d = dprobs[slot, :, tile].reshape(CHUNK // 8, 8, BLK)
            before = peak[:, tile]
            now = jnp.maximum(before, jnp.max(s, axis=0))
            fade = jnp.exp2((before - now) * c)
            e = jnp.exp2((s - now[None]) * c)
            total[:, tile] = total[:, tile] * fade + jnp.sum(e, axis=0)
            weigh[:, tile] = weigh[:, tile] * fade + jnp.sum(e * d, axis=0)
            peak[:, tile] = now

    def own_pair(i, cols):
        return jnp.concatenate([resp[i, :, cols], partner_kv[i, :, cols]], axis=0)

    def own_scores():
        key = lax.broadcasted_iota(jnp.int32, (CHUNK, BLK), 0)
        pos = lax.broadcasted_iota(jnp.int32, (CHUNK, BLK), 1)
        for i in range(NB):
            limit = jnp.where(is_later[i] == 1, CHUNK, BLK)
            seen = jnp.where(key < BLK, pos - key, limit - 1 - key) >= 0
            k_own, v_own = own_pair(i, KEYS), own_pair(i, VALUES)
            for head in range(QPK):
                tile = pl.ds((i * QPK + head) * BLK, BLK)
                scores[OWN, :, tile] = jnp.where(seen, dot(k_own, q_cols[:, tile]), NEG)
                dprobs[OWN, :, tile] = dot(v_own, w_cols[:, tile])
        take_in(OWN)

    def gather_events(s):
        if s == 1:
            arrived(("R", 0, 0), ("L", 0, 1))
            start(("FR", 0), ("FL", 0))
            heard(2)
            spread(0, resp, table_a)
            arrived(("U", 0), ("D", 1))
            start(("FU",), ("FD",), ("R", 3, 0), ("L", 1, 1), ("R", 1, 1), ("L", 3, 0))
            arrived(("R", 0, 1), ("L", 0, 0))
        elif s == 3:
            arrived(("FR", 0), ("FL", 0))
            start(("VU",), ("VD",))
            counts[0].wait_recv()
            count_send[1] = count_send[0] + count_recv[0]
            counts[1].start()
            counts[2].start()
        elif s == 4:
            arrived(("U", 1), ("D", 0))
            start(("R", 1, 0), ("L", 3, 1), ("R", 3, 1), ("L", 1, 0))
        elif s == 6:
            arrived(("R", 3, 0), ("L", 1, 1))
            start(("FR", 3), ("FL", 1))
            arrived(("L", 1, 0))
        elif s == 7:
            arrived(("FU",), ("FD",))
            start(("R", 2, 0), ("L", 2, 1), ("R", 2, 1), ("L", 2, 0))
            every(lambda k: spread_copy(0, resp, table_a, k).wait_recv())
            deliver(1, table_a, send_b, partner_kv)
            arrived(("R", 1, 0), ("R", 1, 1))
        elif s == 8:
            arrived(("L", 3, 1), ("L", 3, 0))
            counts[1].wait_recv()
            counts[2].wait_recv()
            counts[3].start()
        elif s == 9:
            arrived(("R", 3, 1))
        elif s == 11:
            arrived(("R", 2, 0), ("L", 2, 1))
            start(("FR", 2), ("FL", 2))
            arrived(("L", 2, 0))
        elif s == 12:
            arrived(("R", 2, 1))
            counts[3].wait_recv()
            count_send[2] = count_send[1] + count_recv[1] + count_recv[2] + count_recv[3]
            counts[4].start()
        elif s == 13:
            arrived(("VU",), ("FR", 3))
        elif s == 14:
            arrived(("VD",), ("FL", 1))
        elif s == 15:
            every(lambda k: deliver_copy(1, send_b, partner_kv, k).wait_recv())
            own_scores()
            arrived(("FR", 2), ("FL", 2))

    def gather_step(s, carry):
        for k in (1, 3, 4, 6, 7, 8, 9, 11, 12, 13, 14, 15):
            @pl.when(s == k)
            def _(k=k):
                gather_events(k)

        slot = slot_at(GATHER_ORDER, s)
        keys, values = kv[slot, :, KEYS], kv[slot, :, VALUES]
        for n in range(ROWS // WIDE):
            tile = pl.ds(n * WIDE, WIDE)
            scores[slot, :, tile] = dot(keys, q_cols[:, tile])
            dprobs[slot, :, tile] = dot(values, w_cols[:, tile])
            if n:
                take_in(slot, (2 * n - 2, 2 * n - 1))
        take_in(slot, (TILES - 2, TILES - 1))
        return carry

    lax.fori_loop(0, MEMBERS, gather_step, 0)

    for n in range(TILES):
        tile = pl.ds(n * BLK, BLK)
        m = peak[:, tile]
        top = jnp.max(m, axis=0, keepdims=True)
        fade = jnp.exp2((m - top) * c)
        mass = jnp.sum(total[:, tile] * fade, axis=0, keepdims=True)
        delta = jnp.sum(weigh[:, tile] * fade, axis=0, keepdims=True) / mass
        peak[:, tile] = jnp.broadcast_to(top + jnp.log2(mass) * (1.0 / c), (8, BLK))
        weigh[:, tile] = jnp.broadcast_to(delta, (8, BLK))

    def probabilities(slot, tiles=range(TILES)):
        for n in tiles:
            tile = pl.ds(n * BLK, BLK)
            s = scores[slot, :, tile].reshape(CHUNK // 8, 8, BLK)
            d = dprobs[slot, :, tile].reshape(CHUNK // 8, 8, BLK)
            p = jnp.exp2((s - peak[:, tile][None]) * c)
            ds = p * (d - weigh[:, tile][None])
            p_low[:, tile] = p.reshape(CHUNK, BLK).astype(BF16)
            ds_low[:, tile] = ds.reshape(CHUNK, BLK).astype(BF16)

    def add_query_grad(keys, tile):
        dq_cols[:, tile] += lax.dot_general(
            keys, ds_low[:, tile], (((0,), (0,)), ((), ())), preferred_element_type=F32
        )

    def own_grads():
        probabilities(OWN)
        for i in range(NB):
            tile = pl.ds(i * QPK * BLK, QPK * BLK)
            d_keys = dot(ds_low[:, tile], q_rows[tile, :])
            d_values = dot(p_low[:, tile], w_rows[tile, :])
            add_query_grad(own_pair(i, KEYS), tile)
            own_grad[i, :, KEYS] = d_keys[:BLK]
            own_grad[i, :, VALUES] = d_values[:BLK]
            give[i, :, KEYS] = d_keys[BLK:].astype(BF16)
            give[i, :, VALUES] = d_values[BLK:].astype(BF16)

    def joins(a, b, h):
        return (b == 1 and h == 0 and a != 1) or (b == 3 and h == 1 and a != 3)

    def put_by(a, b):
        if b == 0:
            x_sum[a] = g_tmp[...]
        elif (a, b) != (0, 2):
            for h in range(2):
                if joins(a, b, h):
                    g_hold[2 * a + b // 2] = g_tmp[halves[h]]
                else:
                    g_send[a * SIDE + b, halves[h]] = g_tmp[halves[h]].astype(BF16)

    def x_combined(a, h):
        arrived(("gr", a, h), ("gl", a, h))
        half = halves[h]
        return x_sum[a, half] + x_in_l[a, half].astype(F32) + x_in_r[a, half].astype(F32)

    def reduce_event(kind, a=0, h=0):
        half = halves[h]
        if kind == "far":
            if a == 0:
                arrived(("yu",), ("yd",))
                g_send[2] = (g_tmp[...] + z_far[...].astype(F32)).astype(BF16)
            start(("yu",) if a == 1 else ("r", a), ("yd",) if a == 3 else ("l", a))
        elif kind in ("gr", "gl"):
            b, relay, landed = (1, "r", x_rel_a) if kind == "gr" else (3, "l", x_rel_b)
            if joins(a, b, h):
                arrived((relay, a))
                g_send[a * SIDE + b, half] = (g_hold[2 * a + b // 2] + landed[a].astype(F32)).astype(BF16)
            start((kind, a, h))
        elif kind == "z":
            value = x_combined(a, h)
            if (a, h) == (1, 0):
                arrived(("zr",))
                value = value + z_rel[half].astype(F32)
            elif (a, h) == (3, 1):
                arrived(("zl",))
                value = value + z_rel[half].astype(F32)
            z_send[a, half] = value.astype(BF16)
            start({1: ("zu", h), 2: ("zr",) if h == 0 else ("zl",), 3: ("zd", h)}[a])
        elif kind == "own":
            own_grads()
        elif kind == "spread":
            spread(2, give, table_c)
        else:
            every(lambda k: spread_copy(2, give, table_c, k).wait_recv())
            deliver(3, table_c, send_d, partner_grad)

    def reduce_step(p, carry):
        slot = slot_at(REDUCE_ORDER, p)
        keys = kv[slot, :, KEYS]
        d_keys = jnp.zeros((CHUNK, HD), F32)
        d_values = jnp.zeros((CHUNK, HD), F32)
        for n in range(ROWS // WIDE):
            tile = pl.ds(n * WIDE, WIDE)
            probabilities(slot, (2 * n, 2 * n + 1))
            d_keys = d_keys + dot(ds_low[:, tile], q_rows[tile, :])
            d_values = d_values + dot(p_low[:, tile], w_rows[tile, :])
            add_query_grad(keys, tile)
        g_tmp[:, KEYS] = d_keys
        g_tmp[:, VALUES] = d_values

        for k in range(MEMBERS):
            @pl.when(p == k)
            def _(k=k):
                put_by(*REDUCE_ORDER[k])
                for event in REDUCE_EVENTS[k]:
                    reduce_event(*event)

        return carry

    lax.fori_loop(0, MEMBERS, reduce_step, 0)

    counts[4].wait_recv()
    tokens = (count_send[2] + count_recv[4]).astype(F32)
    factor = (LOSS_SCALE * 16 * RESP * CHUNK) / tokens[0:1]
    for i in range(NB):
        for head in range(QPK):
            rows = pl.ds(i * BLK, BLK)
            grads = dq_cols[:, pl.ds((i * QPK + head) * BLK, BLK)]
            grad_query[rows, pl.ds(head * HD, HD)] = (grads.T * (factor * scale)).astype(BF16)

    every(lambda k: deliver_copy(3, send_d, partner_grad, k).wait_recv())
    stream = own_grad[...] + partner_grad[...].astype(F32)
    grad_stream[:, :, KEYS] = (stream[:, :, :HD] * (factor * scale)[None]).astype(BF16)
    grad_stream[:, :, VALUES] = (stream[:, :, HD:] * factor[None]).astype(BF16)

    for h in range(2):
        own = x_combined(0, h)
        arrived(("zu", h), ("zd", h))
        own = own + z_in_l[halves[h]].astype(F32) + z_in_r[halves[h]].astype(F32)
        grad_prompt[halves[h], KEYS] = (own[:, :HD] * (factor * scale)).astype(BF16)
        grad_prompt[halves[h], VALUES] = (own[:, HD:] * factor).astype(BF16)

    for name in copies:
        copies[name].wait_send()
    every(lambda k: spread_copy(0, resp, table_a, k).wait_send())
    every(lambda k: deliver_copy(1, send_b, partner_kv, k).wait_send())
    every(lambda k: spread_copy(2, give, table_c, k).wait_send())
    every(lambda k: deliver_copy(3, send_d, partner_grad, k).wait_send())
    for cp in counts:
        cp.wait_send()


def write_out(query, stream, prompt, query_out, stream_out, prompt_out, sem):
    copies = [
        pltpu.make_async_copy(src, dst, sem.at[k])
        for k, (src, dst) in enumerate(((query, query_out), (stream, stream_out), (prompt, prompt_out)))
    ]
    for cp in copies:
        cp.start()
    for cp in copies:
        cp.wait()


def local(query, resp_kv, prompt_kv, grad_out, rewards, lengths, block_order):
    vmem = pl.BlockSpec(memory_space=pltpu.VMEM)
    hbm = pl.BlockSpec(memory_space=pl.ANY)
    pair = (CHUNK, 2 * HD)
    half = (BLK, 2 * HD)
    blocks = (NB, BLK, 2 * HD)
    pieces = (NB * MEMBERS, 16, HD)
    wide = (CHUNK, QPK * HD)
    grads = pl.pallas_call(
        kernel,
        name="attention_step",
        out_shape=(
            pltpu.VMEM(wide, BF16),
            pltpu.VMEM(blocks, BF16),
            pltpu.VMEM(pair, BF16),
        ),
        in_specs=[hbm] * 7,
        out_specs=(vmem,) * 3,
        scratch_shapes=[
            pltpu.VMEM(wide, BF16),
            pltpu.VMEM(wide, BF16),
            pltpu.VMEM(blocks, BF16),
            pltpu.SMEM((RESP,), F32),
            pltpu.SMEM((RESP,), jnp.int32),
            pltpu.SMEM((NB * MEMBERS,), jnp.int32),
            pltpu.SMEM((NB * MEMBERS,), jnp.int32),
            pltpu.VMEM((MEMBERS, *pair), BF16),
            pltpu.VMEM((MEMBERS + 1, CHUNK, ROWS), F32),
            pltpu.VMEM((MEMBERS + 1, CHUNK, ROWS), F32),
            pltpu.VMEM((ROWS, HD), BF16),
            pltpu.VMEM((ROWS, HD), BF16),
            pltpu.VMEM((HD, ROWS), BF16),
            pltpu.VMEM((HD, ROWS), BF16),
            pltpu.VMEM((8, ROWS), F32),
            pltpu.VMEM((8, ROWS), F32),
            pltpu.VMEM((8, ROWS), F32),
            pltpu.VMEM((CHUNK, ROWS), BF16),
            pltpu.VMEM((CHUNK, ROWS), BF16),
            pltpu.VMEM((HD, ROWS), F32),
            pltpu.VMEM(pair, F32),
            pltpu.VMEM((MEMBERS, *pair), BF16),
            pltpu.VMEM((2 * SIDE, *half), F32),
            pltpu.VMEM((SIDE, *half), BF16),
            pltpu.VMEM((SIDE, *half), BF16),
            pltpu.VMEM((SIDE, *pair), BF16),
            pltpu.VMEM((SIDE, *pair), BF16),
            pltpu.VMEM((SIDE, *pair), F32),
            pltpu.VMEM((SIDE, *pair), BF16),
            pltpu.VMEM(pair, BF16),
            pltpu.VMEM(pair, BF16),
            pltpu.VMEM(pair, BF16),
            pltpu.VMEM(pair, BF16),
            pltpu.VMEM(pieces, BF16),
            pltpu.VMEM(pieces, BF16),
            pltpu.VMEM(blocks, BF16),
            pltpu.VMEM(pieces, BF16),
            pltpu.VMEM(pieces, BF16),
            pltpu.VMEM(blocks, BF16),
            pltpu.VMEM(blocks, BF16),
            pltpu.VMEM(blocks, F32),
            pltpu.VMEM((3, 8, HD), jnp.int32),
            pltpu.VMEM((5, 8, HD), jnp.int32),
            pltpu.SemaphoreType.DMA((N_COPIES,)),
            pltpu.SemaphoreType.DMA((N_COPIES,)),
            pltpu.SemaphoreType.DMA((4, MEMBERS)),
            pltpu.SemaphoreType.DMA((4, MEMBERS)),
            pltpu.SemaphoreType.DMA((5,)),
            pltpu.SemaphoreType.DMA((5,)),
            pltpu.SemaphoreType.DMA((7,)),
            pltpu.SemaphoreType.REGULAR((3,)),
        ],
        compiler_params=pltpu.CompilerParams(
            collective_id=0, has_side_effects=True, vmem_limit_bytes=58 * 2**20
        ),
    )(
        query[0], resp_kv[0].reshape(blocks), prompt_kv[0], grad_out[0],
        rewards[0], lengths[0], block_order[0],
    )
    outs = pl.pallas_call(
        write_out,
        name="write_out",
        out_shape=(
            jax.ShapeDtypeStruct(wide, BF16),
            jax.ShapeDtypeStruct(blocks, BF16),
            jax.ShapeDtypeStruct(pair, BF16),
        ),
        in_specs=[vmem] * 3,
        out_specs=(hbm,) * 3,
        scratch_shapes=[pltpu.SemaphoreType.DMA((3,))],
        compiler_params=pltpu.CompilerParams(vmem_limit_bytes=2**20),
    )(*grads)
    return outs[0][None], outs[1].reshape(1, *pair), outs[2][None]


def solution(mesh):
    rows = P("grp", "seq", None)
    small = P("grp", None)
    return jax.shard_map(
        local,
        mesh=mesh,
        in_specs=(rows, rows, rows, rows, small, small, small),
        out_specs=(rows, rows, rows),
        check_vma=False,
    )
```
